256 devices in a mesh: rep: 8 (over z), ep: 4 (over y), dp: 8 (over x, core).
Axes of the slice: x: 4, y: 4, z: 8, core: 2. Of those that a mesh axis runs over, the one named last changes fastest.
Arguments:
- tok_in: bfloat16 [98304, 384], P(('rep', 'ep', 'dp'))
- tok_grad: bfloat16 [98304, 384], P(('rep', 'ep', 'dp'))
- route_ids: int32 [2, 98304, 2], P(None, ('rep', 'ep', 'dp'))
- gate_vals: float32 [2, 98304, 2], P(None, ('rep', 'ep', 'dp'))
- w_dense: bfloat16 [2, 384, 384], replicated
- w_gate: bfloat16 [2, 8, 384, 2048], P(None, 'ep')
- w_up: bfloat16 [2, 8, 384, 2048], P(None, 'ep')
- w_down: bfloat16 [2, 8, 2048, 384], P(None, 'ep')
Outputs:
- output 1: bfloat16 [98304, 384], P(('rep', 'ep', 'dp'))
- output 2: bfloat16 [98304, 384], P(('rep', 'ep', 'dp'))
- output 3: bfloat16 [2, 384, 384], replicated
- output 4: bfloat16 [2, 8, 384, 2048], P(None, 'ep')
- output 5: bfloat16 [2, 8, 384, 2048], P(None, 'ep')
- output 6: bfloat16 [2, 8, 2048, 384], P(None, 'ep')
All inputs are finite; a program needn't handle non-finite values.
Results may differ from the reference program's by a relative error of at most 0.02.
Values are sent between devices in bfloat16 or wider.
A program may use at most 768 MiB of HBM per device.

```python
import jax
import jax.numpy as jnp
from jax import lax

D = 384
FF = 2048
EXPERTS = 8
TOP = 2
TOKENS = 384
DEVICES = 256
LAYERS = 2
CAPACITY = 2 * TOKENS * TOP // EXPERTS
ROWS = DEVICES * TOKENS


def draw_routes(route_key):
    half_cap = CAPACITY // 2
    key_pair, key_label, key_order = jax.random.split(route_key, 3)
    shifts = jax.random.randint(key_pair, (EXPERTS // 2,), -(half_cap - 2), half_cap - 1)
    shifts = shifts.at[0].set(half_cap - 1)
    counts = jnp.stack([half_cap + shifts, half_cap - shifts], axis=1).reshape(EXPERTS)
    counts = counts.at[0].add(1).at[2].add(-1)
    count_ends = jnp.cumsum(counts)
    positions = jnp.arange(TOKENS * TOP)
    labels = jnp.sum((positions[:, None] >= count_ends[None, :]).astype(jnp.int32), axis=1)
    relabel = jax.random.permutation(key_label, EXPERTS)
    choices = relabel[labels].reshape(TOP, TOKENS).T
    token_order = jax.random.permutation(key_order, TOKENS)
    return choices[token_order].astype(jnp.int32)


def setup_inputs(seed: int = 0) -> dict:
    base_key = jax.random.key(seed)
    key_list = jax.random.split(base_key, 8)
    route_ids = lax.map(draw_routes, jax.random.split(key_list[0], LAYERS * DEVICES)).reshape(LAYERS, ROWS, TOP)
    gate_vals = jax.random.uniform(key_list[1], (LAYERS, ROWS, TOP), jnp.float32, 0.25, 0.75) * TOP ** -0.5
    tok_in = jax.random.normal(key_list[2], (ROWS, D), jnp.float32).astype(jnp.bfloat16)
    tok_grad = jax.random.normal(key_list[3], (ROWS, D), jnp.float32).astype(jnp.bfloat16)
    w_dense = (jax.random.normal(key_list[4], (LAYERS, D, D), jnp.float32) * D ** -0.5).astype(jnp.bfloat16)
    w_gate = (jax.random.normal(key_list[5], (LAYERS, EXPERTS, D, FF), jnp.float32) * D ** -0.5).astype(jnp.bfloat16)
    w_up = (jax.random.normal(key_list[6], (LAYERS, EXPERTS, D, FF), jnp.float32) * D ** -0.5).astype(jnp.bfloat16)
    w_down = (jax.random.normal(key_list[7], (LAYERS, EXPERTS, FF, D), jnp.float32) * FF ** -0.5).astype(jnp.bfloat16)
    return {"tok_in": tok_in, "tok_grad": tok_grad, "route_ids": route_ids, "gate_vals": gate_vals, "w_dense": w_dense, "w_gate": w_gate, "w_up": w_up, "w_down": w_down}


def expert_block(mixed_blk, route_blk, gate_blk, gate_f32, up_f32, down_f32):
    flat_ids = route_blk.reshape(TOKENS * TOP)
    expert_hits = (flat_ids[:, None] == jnp.arange(EXPERTS, dtype=jnp.int32)[None, :]).astype(jnp.int32)
    slot_rank = jnp.sum((jnp.cumsum(expert_hits, axis=0) - 1) * expert_hits, axis=1)
    slot_of = flat_ids * CAPACITY + slot_rank
    copy_of = jnp.full((EXPERTS * CAPACITY,), TOKENS * TOP, jnp.int32).at[slot_of].set(jnp.arange(TOKENS * TOP, dtype=jnp.int32))
    padded = jnp.concatenate([mixed_blk, jnp.zeros((1, D), mixed_blk.dtype)], axis=0)
    rows_in = padded[copy_of // TOP].reshape(EXPERTS, CAPACITY, D).astype(jnp.float32)
    act_gate = jnp.einsum("ecd,edf->ecf", rows_in, gate_f32).astype(jnp.bfloat16)
    act_up = jnp.einsum("ecd,edf->ecf", rows_in, up_f32).astype(jnp.bfloat16)
    hidden = (jax.nn.silu(act_gate.astype(jnp.float32)) * act_up.astype(jnp.float32)).astype(jnp.bfloat16)
    rows_out = jnp.einsum("ecf,efd->ecd", hidden.astype(jnp.float32), down_f32).astype(jnp.bfloat16)
    per_copy = rows_out.reshape(EXPERTS * CAPACITY, D)[slot_of].reshape(TOKENS, TOP, D)
    return jnp.sum(gate_blk[:, :, None] * per_copy.astype(jnp.float32), axis=1)


expert_saved = jax.checkpoint(expert_block)


def layer_forward(tok_in, route_ids, gate_vals, dense_f32, gate_f32, up_f32, down_f32):
    mixed_val = (tok_in.astype(jnp.float32) + jnp.dot(tok_in.astype(jnp.float32), dense_f32)).astype(jnp.bfloat16)

    def block_fn(block_args):
        return expert_saved(block_args[0], block_args[1], block_args[2], gate_f32, up_f32, down_f32)

    mix_sum = lax.map(block_fn, (mixed_val.reshape(DEVICES, TOKENS, D), route_ids.reshape(DEVICES, TOKENS, TOP), gate_vals.reshape(DEVICES, TOKENS, TOP)))
    return (mixed_val.astype(jnp.float32) + mix_sum.reshape(ROWS, D)).astype(jnp.bfloat16)


def reference(tok_in, tok_grad, route_ids, gate_vals, w_dense, w_gate, w_up, w_down):
    def forward_all(tok_start, dense_f32, gate_f32, up_f32, down_f32):
        def layer_step(tok_carry, layer_args):
            return layer_forward(tok_carry, layer_args[0], layer_args[1], layer_args[2], layer_args[3], layer_args[4], layer_args[5]), None

        return lax.scan(layer_step, tok_start, (route_ids, gate_vals, dense_f32, gate_f32, up_f32, down_f32))[0]

    tok_out, pull_back = jax.vjp(forward_all, tok_in, w_dense.astype(jnp.float32), w_gate.astype(jnp.float32), w_up.astype(jnp.float32), w_down.astype(jnp.float32))
    grad_in, grad_dense, grad_gate, grad_up, grad_down = pull_back(tok_grad)
    return (tok_out, grad_in, grad_dense.astype(jnp.bfloat16), grad_gate.astype(jnp.bfloat16), grad_up.astype(jnp.bfloat16), grad_down.astype(jnp.bfloat16))
```

```python
import jax
import jax.numpy as jnp
from jax import lax
from jax.experimental import pallas as pl
from jax.experimental.pallas import tpu as pltpu
from jax.sharding import PartitionSpec as P

TOK_AXES = ("rep", "ep", "dp")
COPY_AXES = ("rep", "dp")
F32 = jnp.float32
BF16 = jnp.bfloat16


def mm(a, b, dims):
    return lax.dot_general(a, b, (dims, ((), ())), preferred_element_type=F32)


LANES = 128
STEP = 16


def shard_copies(local_shards, half, low):
    for k in range(local_shards):
        rows, cols = slice((k % 2) * half, (k % 2 + 1) * half), slice(k // 2 * LANES, (k // 2 + 1) * LANES)
        yield k, 0, half, rows, cols
        yield k, 1, half, rows, cols
        for c in range(half // low):
            yield k, 2 + c, low, slice(k * low, (k + 1) * low), slice(c * LANES, (c + 1) * LANES)


def pack_kernel(half, low, gate_ref, up_ref, down_ref, out_ref):
    for k, piece, size, rows, cols in shard_copies(STEP, half, low):
        src = (gate_ref, up_ref, down_ref)[min(piece, 2)]
        at = piece * half if piece < 2 else 2 * half + (piece - 2) * low
        out_ref[k, at : at + size, :] = src[0, rows, cols]


def unpack_kernel(half, low, in_ref, *refs):
    gate_ref, up_ref, down_ref = refs[-3:]
    for k, piece, size, rows, cols in shard_copies(STEP, half, low):
        dst = (gate_ref, up_ref, down_ref)[min(piece, 2)]
        at = piece * half if piece < 2 else 2 * half + (piece - 2) * low
        dst[0, 0, rows, cols] = in_ref[k, at : at + size, :]


def pack(gate, up, down):
    local, width, ff = gate.shape
    shards = 2 * local * ff // LANES
    half, low = width // 2, local * ff // shards
    per = shards // local // STEP
    wide = pl.BlockSpec((1, width, STEP // 2 * LANES), lambda i: (i // per, 0, i % per))
    tall = pl.BlockSpec((1, STEP * low, width), lambda i: (i // per, i % per, 0))
    rows = 2 * half + width // LANES * low
    return pl.pallas_call(
        lambda *refs: pack_kernel(half, low, *refs),
        grid=(shards // STEP,),
        in_specs=[wide, wide, tall],
        out_specs=pl.BlockSpec((STEP, rows, LANES), lambda i: (i, 0, 0)),
        out_shape=jax.ShapeDtypeStruct((shards, rows, LANES), BF16),
        cost_estimate=pl.CostEstimate(flops=10**8, bytes_accessed=4 * gate.size * 3, transcendentals=0),
        name="pack",
    )(gate, up, down)


def unpack(packed, layer, shapes, into):
    (layers, local, width, ff), shards = shapes[0], packed.shape[0]
    half, low = width // 2, local * ff // shards
    per = shards // local // STEP
    wide = pl.BlockSpec((1, 1, width, STEP // 2 * LANES), lambda i: (layer, i // per, 0, i % per))
    tall = pl.BlockSpec((1, 1, STEP * low, width), lambda i: (layer, i // per, i % per, 0))
    return pl.pallas_call(
        lambda *refs: unpack_kernel(half, low, *refs),
        grid=(shards // STEP,),
        in_specs=[pl.BlockSpec((STEP, packed.shape[1], LANES), lambda i: (i, 0, 0))] + [pl.BlockSpec(memory_space=pl.ANY)] * len(into),
        out_specs=[wide, wide, tall],
        out_shape=[jax.ShapeDtypeStruct(s, BF16) for s in shapes],
        input_output_aliases={1 + i: i for i in range(len(into))},
        cost_estimate=pl.CostEstimate(flops=10**8, bytes_accessed=4 * packed.size, transcendentals=0),
        name=f"unpack_{layer}",
    )(packed, *into)


def slot_tables(route_loc, experts):
    tokens, top_k = route_loc.shape
    capacity = 2 * tokens * top_k // experts
    hits = (route_loc[:, :, None] == jnp.arange(experts, dtype=jnp.int32)).astype(BF16)
    token_hits = jnp.sum(hits, axis=1)
    order = (jnp.arange(tokens)[:, None] > jnp.arange(tokens)[None, :]).astype(BF16)
    before = mm(order, token_hits, ((1,), (0,)))
    rank = jnp.sum(before[:, None, :] * hits.astype(F32), axis=2).astype(jnp.int32)
    slot_of = route_loc * capacity + rank
    slots = jnp.arange(experts * capacity, dtype=jnp.int32)
    return (slots[None, :, None] == slot_of.T[:, None, :]).astype(BF16)


def layer_forward(tok_loc, pick, gate_loc, dense_w, gate_w, up_w, down_w, ep_size):
    tokens, top_k = gate_loc.shape
    model_width = tok_loc.shape[1]
    experts = gate_w.shape[0] * ep_size
    capacity = 2 * tokens * top_k // experts
    mixed_val = (tok_loc.astype(F32) + mm(tok_loc, dense_w, ((1,), (0,)))).astype(BF16)
    send_buf = mm(pick[0] + pick[1], mixed_val, ((1,), (0,))).astype(BF16).reshape(experts, capacity, model_width)
    expert_in = lax.all_to_all(send_buf, "ep", 0, 1, tiled=True)
    act_gate = jnp.einsum("end,edf->enf", expert_in, gate_w, preferred_element_type=F32).astype(BF16)
    act_up = jnp.einsum("end,edf->enf", expert_in, up_w, preferred_element_type=F32).astype(BF16)
    hidden = (jax.nn.silu(act_gate.astype(F32)) * act_up.astype(F32)).astype(BF16)
    expert_out = jnp.einsum("enf,efd->end", hidden, down_w, preferred_element_type=F32).astype(BF16)
    returned = lax.all_to_all(expert_out, "ep", 1, 0, tiled=True).reshape(experts * capacity, model_width)
    mix_sum = gate_loc[:, 0:1] * mm(pick[0], returned, ((0,), (0,))) + gate_loc[:, 1:2] * mm(pick[1], returned, ((0,), (0,)))
    tok_out = (mixed_val.astype(F32) + mix_sum).astype(BF16)
    return tok_out, (tok_loc, expert_in, act_gate, act_up, hidden)


def send_gradient(grad_out, pick, gate_loc, experts):
    slots, tokens = pick.shape[1:]
    grad_f = grad_out.astype(F32)
    scaled = jnp.concatenate([(gate_loc[:, 0:1] * grad_f).astype(BF16), (gate_loc[:, 1:2] * grad_f).astype(BF16)], axis=0)
    both = jnp.concatenate([pick[0], pick[1]], axis=1)
    rows = mm(both, scaled, ((1,), (0,))).astype(BF16)
    return lax.all_to_all(rows.reshape(experts, slots // experts, grad_out.shape[1]), "ep", 0, 1, tiled=True)


def layer_backward(grad_out, grad_exp_out, pick, dense_w, gate_w, up_w, down_w, layer_saved, ep_size, gathered):
    tok_loc, expert_in, act_gate, act_up, hidden = layer_saved
    model_width = grad_out.shape[1]
    grad_hidden = jnp.einsum("end,efd->enf", grad_exp_out, down_w, preferred_element_type=F32)
    gate_f = act_gate.astype(F32)
    sig_gate = jax.nn.sigmoid(gate_f)
    grad_up_act = (grad_hidden * gate_f * sig_gate).astype(BF16)
    grad_gate_act = (grad_hidden * act_up.astype(F32) * sig_gate * (1.0 + gate_f * (1.0 - sig_gate))).astype(BF16)
    grad_exp_in = (jnp.einsum("enf,edf->end", grad_gate_act, gate_w, preferred_element_type=F32) + jnp.einsum("enf,edf->end", grad_up_act, up_w, preferred_element_type=F32)).astype(BF16)
    grad_back = lax.all_to_all(grad_exp_in, "ep", 1, 0, tiled=True).reshape(pick.shape[1], model_width)
    grad_down = jnp.einsum("enf,end->efd", hidden, grad_exp_out, preferred_element_type=F32).astype(BF16)
    grad_gate = jnp.einsum("end,enf->edf", expert_in, grad_gate_act, preferred_element_type=F32).astype(BF16)
    grad_up = jnp.einsum("end,enf->edf", expert_in, grad_up_act, preferred_element_type=F32).astype(BF16)
    packed = pack(grad_gate, grad_up, grad_down)
    if gathered is not None:
        packed, gathered = lax.optimization_barrier((packed, gathered))
    summed = lax.psum_scatter(packed, COPY_AXES, scatter_dimension=0, tiled=False)
    grad_mixed = grad_out.astype(F32) + mm(pick[0] + pick[1], grad_back, ((0,), (0,)))
    grad_mixed_bf = grad_mixed.astype(BF16)
    grad_dense = mm(tok_loc, grad_mixed_bf, ((0,), (0,))).astype(BF16)
    grad_tok = (grad_mixed + mm(grad_mixed_bf, dense_w, ((1,), (1,)))).astype(BF16)
    return grad_tok, grad_dense, summed, gathered


def sum_dense(grads):
    rows, width = grads.shape
    part = grads
    for axis in ("dp", "rep"):
        pieces = lax.all_to_all(part.reshape(lax.axis_size(axis), -1, width), axis, 0, 0, tiled=True)
        part = jnp.sum(pieces.astype(F32), axis=0).astype(BF16)
    part = jnp.sum(lax.all_gather(part, "ep", axis=0).astype(F32), axis=0).astype(BF16)
    for axis in ("rep", "dp"):
        part = lax.all_gather(part, axis, axis=0, tiled=True)
    return part


def solution(mesh):
    ep_size = mesh.shape["ep"]
    tok_spec = P(TOK_AXES, None)
    route_spec = P(None, TOK_AXES, None)
    expert_spec = P(None, "ep", None, None)
    whole_spec = P(None, None, None)

    def device_step(tok_in, tok_grad, route_ids, gate_vals, w_dense, w_gate, w_up, w_down):
        layers, model_width = w_dense.shape[:2]
        local, ff = w_gate.shape[1], w_gate.shape[3]
        experts = local * ep_size
        picks = [slot_tables(route_ids[i], experts) for i in range(layers)]
        current = tok_in
        saved_all = []
        for i in range(layers):
            current, layer_saved = layer_forward(current, picks[i], gate_vals[i], w_dense[i], w_gate[i], w_up[i], w_down[i], ep_size)
            saved_all.append(layer_saved)
        grad_cur = tok_grad
        dense, summed, gathered, grads = [None] * layers, None, None, ()
        shapes = [w_gate.shape, w_up.shape, w_down.shape]
        for i in reversed(range(layers)):
            sent = send_gradient(grad_cur, picks[i], gate_vals[i], experts)
            if summed is not None:
                sent, summed = lax.optimization_barrier((sent, summed))
                gathered = lax.all_gather(summed, COPY_AXES, axis=0)
            grad_cur, dense[i], summed, gathered = layer_backward(grad_cur, sent, picks[i], w_dense[i], w_gate[i], w_up[i], w_down[i], saved_all[i], ep_size, gathered)
            if gathered is not None:
                grads = unpack(gathered, i + 1, shapes, grads)
        grad_cur, dense, current, summed = lax.optimization_barrier((grad_cur, dense, current, summed))
        grad_dense = sum_dense(jnp.concatenate(dense, axis=0)).reshape(layers, model_width, model_width)
        grads = unpack(lax.all_gather(summed, COPY_AXES, axis=0), 0, shapes, grads)
        return current, grad_cur, grad_dense, *grads

    return jax.shard_map(device_step, mesh=mesh, in_specs=(tok_spec, tok_spec, route_spec, route_spec, whole_spec, expert_spec, expert_spec, expert_spec), out_specs=(tok_spec, tok_spec, whole_spec, expert_spec, expert_spec, expert_spec), check_vma=False)
```
